32 devices in a mesh: leaf: 8 (over z, y), hand: 4 (over x, core).
Axes of the slice: x: 2, y: 2, z: 4, core: 2. Of those that a mesh axis runs over, the one named last changes fastest.
Arguments:
- opp_range: float32 [1024], P('hand'), may hold values from 0.1 to 1
- br_range: float32 [1024], P('hand'), may hold values from 0.001 to 1
- up_weight: bfloat16 [4, 256, 1024], P(None, 'leaf', 'hand'), may hold values from 0.29882812 to 1
- up_parent: int32 [3, 256], replicated, may hold values from 0 to 255
- board_cards: int32 [768, 5], P('leaf'), may hold values from 0 to 51, as said below
- hand_rank: int32 [768, 1024], P('leaf'), may hold values from 0 to 7461
- root_parent: int32 [768], P('leaf'), may hold values from 0 to 255
- br_actions: int32 [768], P('leaf'), may hold values from 1 to 8
- opp_actions: int32 [768, 8], P('leaf'), may hold values from 1 to 8
- leaf_kind: int32 [768, 8, 8], P('leaf'), may hold values from 0 to 1
- leaf_stake: int32 [768, 8, 8], P('leaf'), may hold values from 1 to 400
- opp_weight: bfloat16 [768, 8, 8, 1024], P('leaf', None, None, 'hand'), may hold values from 0.049804688 to 1
Outputs:
- level_values: float32 [4, 256, 1024], P(None, 'leaf', 'hand')
- root_value: float32 [1024], P('hand')
- best_value: float32 [], replicated
The draws below stay inside these ranges and needn't reach their ends.
Inputs may be any that keep to these rules, and one draw needn't show every extreme that they name: `board_cards`: five different cards for each subtree.
All inputs are finite; a program needn't handle non-finite values.
Results may differ from the reference program's by a relative error of at most 0.0003.
Values may be sent and summed in bfloat16 or wider, within the bound.
A program may use at most 128 MiB of HBM per device.

```python
import math
import jax
import jax.numpy as jnp
import numpy as np
from jax import lax

HANDS = 1024
ACT = 8
UP = 4
UNODES = 256
SUBTREES = 768


def pick_cards(subkey):
    return jax.random.permutation(subkey, 52)[:5]


def draw_board_cards(key, part):
    subkeys = jax.random.split(jax.random.fold_in(key, 17), SUBTREES)
    return jax.vmap(pick_cards)(subkeys).astype(jnp.int32)


def set_ends(values, stream_key, least, high):
    shape = values.shape
    index_at = [jax.random.randint(jax.random.fold_in(stream_key, axis), (), 0, shape[axis]) for axis in range(len(shape))]
    values = values.at[tuple(index_at)].set(least)
    longest = shape.index(max(shape))
    index_at[longest] = (index_at[longest] + 1) % shape[longest]
    return values.at[tuple(index_at)].set(high)


def block_scale(key, extent, pieces, least, high):
    level, own = 1.0, jax.random.fold_in(key, 6)
    for dim, parts in pieces:
        steps = jnp.exp(jax.random.uniform(jax.random.fold_in(own, dim), (parts,), jnp.float32, least / len(pieces), high / len(pieces)))
        level = level * jnp.repeat(steps, extent[dim] // parts).reshape([-1 if axis == dim else 1 for axis in range(len(extent))])
    return level


def setup_inputs(seed: int = 0) -> dict:
    arg_keys = jax.random.split(jax.random.key(seed), 13)
    return {
        "opp_range": jnp.clip(jnp.exp(math.log(1.0) - 2.3025851 * jax.random.uniform(arg_keys[0], (HANDS,), jnp.float32) ** block_scale(arg_keys[0], (HANDS,), ((0, 4),), -0.2, 0.2)), 0.1, 1.0),
        "br_range": jnp.clip(jnp.exp(math.log(1.0) - 6.9077552 * jax.random.uniform(arg_keys[1], (HANDS,), jnp.float32) ** block_scale(arg_keys[1], (HANDS,), ((0, 4),), -0.2, 0.2)), 0.001, 1.0),
        "up_weight": jnp.clip(jnp.exp(math.log(1.0) - 1.2078867 * jax.random.uniform(arg_keys[2], (UP, UNODES, HANDS), jnp.float32) ** block_scale(arg_keys[2], (UP, UNODES, HANDS), ((1, 8), (2, 4)), -0.2, 0.2)), 0.29882812, 1.0).astype(jnp.bfloat16),
        "up_parent": set_ends(jax.random.randint(arg_keys[3], (UP - 1, UNODES), 0, UNODES), jax.random.fold_in(arg_keys[3], 1), 0, UNODES - 1).astype(jnp.int32),
        "board_cards": draw_board_cards(jax.random.fold_in(arg_keys[12], 71), 0),
        "hand_rank": set_ends(jax.random.randint(arg_keys[5], (SUBTREES, HANDS), 0, 7462), jax.random.fold_in(arg_keys[5], 1), 0, 7461).astype(jnp.int32),
        "root_parent": set_ends(jax.random.randint(arg_keys[6], (SUBTREES,), 0, UNODES), jax.random.fold_in(arg_keys[6], 1), 0, UNODES - 1).astype(jnp.int32),
        "br_actions": set_ends(jax.random.randint(arg_keys[7], (SUBTREES,), 1, ACT + 1), jax.random.fold_in(arg_keys[7], 1), 1, ACT).astype(jnp.int32),
        "opp_actions": set_ends(jax.random.randint(arg_keys[8], (SUBTREES, ACT), 1, ACT + 1), jax.random.fold_in(arg_keys[8], 1), 1, ACT).astype(jnp.int32),
        "leaf_kind": set_ends(jax.random.randint(arg_keys[9], (SUBTREES, ACT, ACT), 0, 2), jax.random.fold_in(arg_keys[9], 1), 0, 1).astype(jnp.int32),
        "leaf_stake": set_ends(jax.random.randint(arg_keys[10], (SUBTREES, ACT, ACT), 1, 401), jax.random.fold_in(arg_keys[10], 1), 1, 400).astype(jnp.int32),
        "opp_weight": jnp.clip(jnp.exp(math.log(1.0) - 2.9996462 * jax.random.uniform(arg_keys[11], (SUBTREES, ACT, ACT, HANDS), jnp.float32) ** block_scale(arg_keys[11], (SUBTREES, ACT, ACT, HANDS), ((0, 8), (3, 4)), -0.2, 0.2)), 0.049804688, 1.0).astype(jnp.bfloat16),
    }


PAYOFF_UNIT = 1.0 / 4096.0


def hand_cards(number):
    low_list = []
    high_list = []
    for low_card in range(52):
        for high_card in range(low_card + 1, 52):
            low_list.append(low_card)
            high_list.append(high_card)
    chosen = (np.arange(number) * 1326) // number
    return np.array(low_list, np.int32)[chosen], np.array(high_list, np.int32)[chosen]


def no_shared(low_rows, high_rows, low_cols, high_cols):
    apart_mask = (low_rows[:, None] != low_cols[None, :]) & (low_rows[:, None] != high_cols[None, :])
    apart_mask = apart_mask & (high_rows[:, None] != low_cols[None, :]) & (high_rows[:, None] != high_cols[None, :])
    return apart_mask.astype(jnp.float32)


def board_compat(board_cards, low_cols, high_cols):
    hits = (board_cards[:, :, None] == low_cols[None, None, :]) | (board_cards[:, :, None] == high_cols[None, None, :])
    return 1.0 - jnp.any(hits, axis=1).astype(jnp.float32)


def board_values(packed, noshare):
    root_row, compat_row, rank_row, opp_count, br_count, kind_rows, stake_rows, weight_rows = packed
    legal_mask = (jnp.arange(ACT)[None, :] < opp_count[:, None]).astype(jnp.float32)
    weighted = weight_rows.astype(jnp.float32) * legal_mask[:, :, None]
    probability = weighted / jnp.sum(weighted, axis=1, keepdims=True)
    leaf_reach = (root_row[None, None, :] * probability).astype(jnp.bfloat16).reshape(ACT * ACT, HANDS)
    reach_wide = leaf_reach.astype(jnp.float32)
    order_sign = jnp.sign(rank_row[None, :] - rank_row[:, None]).astype(jnp.float32) * noshare
    showdown = jnp.dot(reach_wide, order_sign, precision=lax.Precision.HIGHEST)
    folded = jnp.dot(reach_wide, noshare, precision=lax.Precision.HIGHEST)
    stake_scaled = stake_rows.reshape(-1).astype(jnp.float32) * PAYOFF_UNIT
    payoff = jnp.where(kind_rows.reshape(-1)[:, None] == 1, showdown, folded) * stake_scaled[:, None] * compat_row[None, :]
    per_node = jnp.sum(payoff.reshape(ACT, ACT, HANDS), axis=1)
    allowed = jnp.arange(ACT)[:, None] < br_count
    return jnp.max(jnp.where(allowed, per_node, -1e30), axis=0)


def reference(opp_range, br_range, up_weight, up_parent, board_cards, hand_rank, root_parent, br_actions, opp_actions, leaf_kind, leaf_stake, opp_weight):
    low_np, high_np = hand_cards(HANDS)
    low_all = jnp.asarray(low_np)
    high_all = jnp.asarray(high_np)
    compat = board_compat(board_cards, low_all, high_all)
    noshare = no_shared(low_all, high_all, low_all, high_all)
    reach_now = opp_range[None, :] * up_weight[0].astype(jnp.float32)
    for level_id in range(1, UP):
        reach_now = jnp.take(reach_now, up_parent[level_id - 1], axis=0) * up_weight[level_id].astype(jnp.float32)
    root_reach = jnp.take(reach_now, root_parent, axis=0) * compat

    def one_board(packed):
        return board_values(packed, noshare)

    sub_value = lax.map(one_board, (root_reach, compat, hand_rank, opp_actions, br_actions, leaf_kind, leaf_stake, opp_weight))
    level_sum = jax.ops.segment_sum(sub_value, root_parent, num_segments=UNODES)
    level_list = [level_sum]
    for level_id in range(UP - 1, 0, -1):
        level_sum = jax.ops.segment_sum(level_sum, up_parent[level_id - 1], num_segments=UNODES)
        level_list.insert(0, level_sum)
    level_values = jnp.stack(level_list)
    root_value = jnp.sum(level_values[0], axis=0) / UNODES
    best_value = jnp.sum(br_range * root_value) / jnp.sum(br_range)
    return level_values, root_value, best_value
```

```python
import functools

import jax
import jax.numpy as jnp
import numpy as np
from jax import lax
from jax.experimental import pallas as pl
from jax.experimental.pallas import tpu as pltpu
from jax.sharding import PartitionSpec as P

PAYOFF_UNIT = 1.0 / 4096.0
VMEM_LIMIT = 60 * 1024 * 1024
F32 = jnp.float32
BF16 = jnp.bfloat16


def hand_cards(number):
    low_list = []
    high_list = []
    for low_card in range(52):
        for high_card in range(low_card + 1, 52):
            low_list.append(low_card)
            high_list.append(high_card)
    chosen = np.arange(number) * 1326 // number
    cards = np.zeros((8, number), np.float32)
    cards[0] = np.array(low_list)[chosen]
    cards[1] = np.array(high_list)[chosen]
    return cards


def vmem():
    return pl.BlockSpec(memory_space=pltpu.VMEM)


def hbm():
    return pl.BlockSpec(memory_space=pl.ANY)


def greet(axes_sizes):
    barrier = pltpu.get_barrier_semaphore()
    count = 0
    for axis, size in axes_sizes:
        me = lax.axis_index(axis)
        for dist in range(1, size):
            pl.semaphore_signal(
                barrier,
                inc=1,
                device_id={axis: lax.rem(me + dist, size)},
                device_id_type=pl.DeviceIdType.MESH,
            )
            count += 1
    pl.semaphore_wait(barrier, count)


def push(axis, size, source, target, send_sem, recv_sem):
    me = lax.axis_index(axis)
    copies = []
    for dist in range(1, size):
        peer = lax.rem(me + dist, size)
        copy = pltpu.make_async_remote_copy(
            src_ref=source(peer),
            dst_ref=target,
            send_sem=send_sem.at[dist - 1],
            recv_sem=recv_sem.at[dist - 1],
            device_id={axis: peer},
            device_id_type=pl.DeviceIdType.MESH,
        )
        copy.start()
        copies.append(copy)
    return copies


def sems(size):
    return pltpu.SemaphoreType.DMA((max(size - 1, 1),))


def gather_kernel(leafs, w_ref, a_ref, w_out, a_out, ws, wr, as_, ar, local_sem):
    me = lax.axis_index("leaf")
    greet((("leaf", leafs),))
    own = [
        pltpu.make_async_copy(w_ref, w_out.at[me], local_sem.at[0]),
        pltpu.make_async_copy(a_ref, a_out.at[me], local_sem.at[1]),
    ]
    for copy in own:
        copy.start()
    copies = push("leaf", leafs, lambda peer: w_ref, w_out.at[me], ws, wr)
    copies += push("leaf", leafs, lambda peer: a_ref, a_out.at[me], as_, ar)
    for copy in own + copies:
        copy.wait()


def gather_upper(weights, ancestors, leafs):
    return pl.pallas_call(
        functools.partial(gather_kernel, leafs),
        out_shape=(
            jax.ShapeDtypeStruct((leafs,) + weights.shape, weights.dtype),
            jax.ShapeDtypeStruct((leafs,) + ancestors.shape, ancestors.dtype),
        ),
        in_specs=[vmem(), vmem()],
        out_specs=(vmem(), vmem()),
        scratch_shapes=[sems(leafs), sems(leafs), sems(leafs), sems(leafs), pltpu.SemaphoreType.DMA((2,))],
        compiler_params=pltpu.CompilerParams(
            collective_id=0, has_side_effects=True, vmem_limit_bytes=VMEM_LIMIT
        ),
        name="gather_upper",
    )(weights, ancestors)


def fold_kernel(levels, actions, anc_ref, board_ref, range_ref, cards_ref, upper_ref, stake_ref, weight_ref, out_ref, reach_ref):
    block = stake_ref.shape[0]
    step = pl.program_id(0)

    @pl.when(step == 0)
    def _():
        boards = anc_ref.shape[0]
        leafs, _, nodes_dev, hands = upper_ref.shape
        node_ids = lax.broadcasted_iota(jnp.int32, (boards, leafs * nodes_dev), 1)
        reach = jnp.broadcast_to(range_ref[...], (boards, hands))
        for level in range(levels):
            pick = jnp.where(anc_ref[:, level : level + 1] == node_ids, 1.0, 0.0).astype(BF16)
            table = upper_ref[:, level].reshape(leafs * nodes_dev, hands)
            reach = reach * jnp.dot(pick, table, preferred_element_type=F32)
        low = cards_ref[0:1, :]
        high = cards_ref[1:2, :]
        free = jnp.ones((boards, hands), F32)
        for card in range(5):
            column = board_ref[:, card : card + 1]
            free = jnp.where((column == low) | (column == high), 0.0, free)
        reach_ref[...] = reach * free

    span = actions * actions
    diagonal = lax.broadcasted_iota(jnp.int32, (actions, span), 0) == (
        lax.broadcasted_iota(jnp.int32, (actions, span), 1) // actions
    )
    for i in range(block):
        stake = jnp.broadcast_to(stake_ref[i : i + 1, :], (actions, span))
        stake = jnp.where(diagonal, stake, 0.0)
        legal = jnp.where(stake != 0.0, 1.0, 0.0)
        shown = jnp.maximum(stake, 0.0)
        fold = jnp.maximum(-stake, 0.0)
        shown_hi = jnp.floor(shown * 0.5) * 2.0
        fold_hi = jnp.floor(fold * 0.5) * 2.0
        rows = jnp.concatenate([legal, shown_hi, shown - shown_hi, fold_hi, fold - fold_hi], axis=0)
        sums = jnp.dot(rows.astype(BF16), weight_ref[i], preferred_element_type=F32)
        scale = reach_ref[pl.ds(step * block + i, 1), :] / sums[0:actions]
        part = [sums[k * actions : (k + 1) * actions] for k in range(5)]
        both = jnp.concatenate([(part[1] + part[2]) * scale, (part[3] + part[4]) * scale], axis=0)
        out_ref[2 * actions * i : 2 * actions * (i + 1), :] = both.astype(BF16)


def fold_reach(anc_columns, boards, opp_range, cards_mine, upper, stakes, weights, levels, actions):
    count, span, hands = weights.shape
    block = 8
    whole = lambda array: pl.BlockSpec(array.shape, lambda i: (0,) * array.ndim)
    return pl.pallas_call(
        functools.partial(fold_kernel, levels, actions),
        grid=(count // block,),
        out_shape=jax.ShapeDtypeStruct((count * 2 * actions, hands), BF16),
        in_specs=[
            whole(anc_columns),
            whole(boards),
            whole(opp_range),
            whole(cards_mine),
            whole(upper),
            pl.BlockSpec((block, span), lambda i: (i, 0)),
            pl.BlockSpec((block, span, hands), lambda i: (i, 0, 0)),
        ],
        out_specs=pl.BlockSpec((block * 2 * actions, hands), lambda i: (i, 0)),
        scratch_shapes=[pltpu.VMEM((count, hands), F32)],
        compiler_params=pltpu.CompilerParams(vmem_limit_bytes=VMEM_LIMIT),
        name="fold_reach",
    )(anc_columns, boards, opp_range, cards_mine, upper, stakes, weights)


def swap_kernel(hands, x_ref, out_ref, send, recv, local_sem):
    me = lax.axis_index("hand")
    greet((("hand", hands),))
    own = pltpu.make_async_copy(x_ref.at[me], out_ref.at[me], local_sem)
    own.start()
    for copy in push("hand", hands, lambda peer: x_ref.at[peer], out_ref.at[me], send, recv):
        copy.wait()
    own.wait()


def swap_hands(x, hands):
    return pl.pallas_call(
        functools.partial(swap_kernel, hands),
        out_shape=jax.ShapeDtypeStruct(x.shape, x.dtype),
        in_specs=[vmem()],
        out_specs=vmem(),
        scratch_shapes=[sems(hands), sems(hands), pltpu.SemaphoreType.DMA(())],
        compiler_params=pltpu.CompilerParams(
            collective_id=1, has_side_effects=True, vmem_limit_bytes=VMEM_LIMIT
        ),
        name="swap_hands",
    )(x)


def value_kernel(actions, place_ref, br_ref, rank_ref, board_ref, cards_ref, reach_ref, out_ref, apart_ref):
    parts, rows_all, width = reach_ref.shape
    block, hands = rank_ref.shape
    step = pl.program_id(0)
    low = cards_ref[0:1, :]
    high = cards_ref[1:2, :]

    @pl.when(step == 0)
    def _():
        columns = cards_ref[...].T
        for part in range(parts):
            rows = slice(part * width, (part + 1) * width)
            low_col = columns[rows, 0:1]
            high_col = columns[rows, 1:2]
            hit = (low_col == low) | (low_col == high) | (high_col == low) | (high_col == high)
            apart_ref[rows, :] = jnp.where(hit, 0.0, 1.0).astype(BF16)

    free = jnp.ones((block, hands), F32)
    for card in range(5):
        column = board_ref[:, card : card + 1]
        free = jnp.where((column == low) | (column == high), 0.0, free)

    folded = jnp.zeros((rows_all, hands), F32)
    for part in range(parts):
        folded = folded + jnp.dot(
            reach_ref[part], apart_ref[part * width : (part + 1) * width, :], preferred_element_type=F32
        )
    rank_columns = rank_ref[...].T
    action_ids = lax.broadcasted_iota(jnp.int32, (actions, 1), 0)
    both = 2 * actions
    best_rows = []
    for i in range(block):
        row = rank_ref[i : i + 1, :]
        shown = jnp.zeros((both, hands), F32)
        for part in range(parts):
            rows = slice(part * width, (part + 1) * width)
            apart = apart_ref[rows, :]
            order = (row - rank_columns[rows, i : i + 1]).astype(BF16)
            order = jnp.minimum(jnp.maximum(order, -apart), apart)
            shown = shown + jnp.dot(
                reach_ref[part, i * both : (i + 1) * both, :], order, preferred_element_type=F32
            )
        per_node = shown[0:actions] + folded[i * both + actions : (i + 1) * both]
        allowed = action_ids < br_ref[place_ref[0] + step * block + i]
        best_rows.append(jnp.max(jnp.where(allowed, per_node, -1e30), axis=0, keepdims=True))
    best = jnp.concatenate(best_rows, axis=0) * (free * PAYOFF_UNIT)
    for part in range(parts):
        out_ref[part] = best[:, part * width : (part + 1) * width]


def subtree_values(place, br_actions, ranks, boards, cards, reach, actions):
    parts, rows, width = reach.shape
    hands = ranks.shape[1]
    mine = rows // (2 * actions)
    block = 8
    steps = mine // block
    index = lambda i, place, br: (lax.div(place[0], block) + i, 0)
    return pl.pallas_call(
        functools.partial(value_kernel, actions),
        grid_spec=pltpu.PrefetchScalarGridSpec(
            num_scalar_prefetch=2,
            grid=(steps,),
            in_specs=[
                pl.BlockSpec((block, hands), index),
                pl.BlockSpec((block, boards.shape[1]), index),
                pl.BlockSpec(cards.shape, lambda i, place, br: (0, 0)),
                pl.BlockSpec((parts, block * 2 * actions, width), lambda i, place, br: (0, i, 0)),
            ],
            out_specs=pl.BlockSpec((parts, block, width), lambda i, place, br: (0, i, 0)),
            scratch_shapes=[pltpu.VMEM((hands, hands), BF16)],
        ),
        out_shape=jax.ShapeDtypeStruct((parts, mine, width), F32),
        compiler_params=pltpu.CompilerParams(vmem_limit_bytes=VMEM_LIMIT),
        name="subtree_values",
    )(place, br_actions, ranks, boards, cards, reach)


def level_kernel(
    hands, leafs, levels, nodes_dev, x_ref, anc_ref, br_ref, level_out, root_out, best_out,
    mine, every, tally, send1, recv1, send2, recv2, send3, recv3, local_sem,
):
    hand = lax.axis_index("hand")
    leaf = lax.axis_index("leaf")
    greet((("hand", hands), ("leaf", leafs)))
    own = pltpu.make_async_copy(x_ref.at[hand], mine.at[hand], local_sem)
    own.start()
    for copy in push("hand", hands, lambda peer: x_ref.at[peer], mine.at[hand], send1, recv1):
        copy.wait()
    own.wait()
    copies = push("leaf", leafs, lambda peer: mine, every.at[leaf], send2, recv2)
    own = pltpu.make_async_copy(mine, every.at[leaf], local_sem)
    own.start()
    own.wait()
    for copy in copies:
        copy.wait()
    width = x_ref.shape[2]
    boards = mine.shape[0] * mine.shape[1]
    node_ids = leaf * nodes_dev + lax.broadcasted_iota(jnp.int32, (nodes_dev, boards), 0)

    def add_leaf(source, carry):
        sums, total = carry
        values = every[source].reshape(boards, width)
        coarse = values.astype(BF16)
        fine = (values - coarse.astype(F32)).astype(BF16)
        lines = anc_ref[source]
        pick = jnp.concatenate(
            [jnp.where(lines[k : k + 1, 0:boards] == node_ids, 1.0, 0.0) for k in range(levels)], axis=0
        ).astype(BF16)
        sums = sums + jnp.dot(pick, coarse, preferred_element_type=F32)
        sums = sums + jnp.dot(pick, fine, preferred_element_type=F32)
        return sums, total + jnp.sum(values, axis=0, keepdims=True)

    start = (jnp.zeros((levels * nodes_dev, width), F32), jnp.zeros((1, width), F32))
    sums, total = lax.fori_loop(0, leafs, add_leaf, start)
    for k in range(levels):
        level_out[k] = sums[k * nodes_dev : (k + 1) * nodes_dev]
    root = total / (nodes_dev * leafs)
    root_out[...] = root
    weight = br_ref[...]
    pair = jnp.concatenate(
        [
            jnp.broadcast_to(jnp.sum(weight * root, axis=1, keepdims=True), (8, 128)),
            jnp.broadcast_to(jnp.sum(weight, axis=1, keepdims=True), (8, 128)),
        ],
        axis=0,
    )
    tally[hand] = pair
    copies = push("hand", hands, lambda peer: tally.at[hand], tally.at[hand], send3, recv3)
    for copy in copies:
        copy.wait()
    both = jnp.sum(tally[...], axis=0)
    best_out[...] = both[0:8] / both[8:16]


def level_sums(values, ancestors, br_range, hands, leafs, levels, nodes_dev):
    _, mine, width = values.shape
    return pl.pallas_call(
        functools.partial(level_kernel, hands, leafs, levels, nodes_dev),
        out_shape=(
            jax.ShapeDtypeStruct((levels, nodes_dev, width), F32),
            jax.ShapeDtypeStruct((1, width), F32),
            jax.ShapeDtypeStruct((8, 128), F32),
        ),
        in_specs=[vmem(), vmem(), vmem()],
        out_specs=(vmem(), vmem(), vmem()),
        scratch_shapes=[
            pltpu.VMEM((hands, mine, width), F32),
            pltpu.VMEM((leafs, hands, mine, width), F32),
            pltpu.VMEM((hands, 16, 128), F32),
            sems(hands), sems(hands), sems(leafs), sems(leafs), sems(hands), sems(hands),
            pltpu.SemaphoreType.DMA(()),
        ],
        compiler_params=pltpu.CompilerParams(
            collective_id=2, has_side_effects=True, vmem_limit_bytes=VMEM_LIMIT
        ),
        name="level_sums",
    )(values, ancestors, br_range)


def local(
    opp_range,
    br_range,
    up_weight,
    up_parent,
    board_cards,
    hand_rank,
    root_parent,
    br_actions,
    opp_actions,
    leaf_kind,
    leaf_stake,
    opp_weight,
):
    levels, nodes_dev, hands_dev = up_weight.shape
    boards_dev, hands_all = hand_rank.shape
    actions = opp_actions.shape[1]
    leafs = lax.axis_size("leaf")
    hands = lax.axis_size("hand")
    hand = lax.axis_index("hand")
    mine = boards_dev // hands
    cards = jnp.asarray(hand_cards(hands_all))
    cards_mine = lax.dynamic_slice_in_dim(cards, hand * hands_dev, hands_dev, 1)
    boards = board_cards.astype(F32)

    node_ids = jnp.arange(up_parent.shape[1])
    chain = [root_parent]
    for level in range(levels - 2, -1, -1):
        chosen = jnp.where(chain[0][:, None] == node_ids[None, :], up_parent[level][None, :], 0)
        chain.insert(0, jnp.sum(chosen, axis=1))
    anc_columns = jnp.stack(chain, axis=1)
    lanes = -(-boards_dev // 128) * 128
    anc_rows = jnp.pad(jnp.stack(chain, axis=0), ((0, -levels % 8), (0, lanes - boards_dev)))

    upper, ancestors = gather_upper(up_weight, anc_rows, leafs)

    signed = jnp.where(leaf_kind == 1, leaf_stake, -leaf_stake)
    legal = jnp.arange(actions)[None, None, :] < opp_actions[:, :, None]
    stakes = jnp.where(legal, signed, 0).astype(F32).reshape(boards_dev, actions * actions)
    weights = opp_weight.reshape(boards_dev, actions * actions, hands_dev)
    folded = fold_reach(
        anc_columns, boards, opp_range[None, :], cards_mine, upper, stakes, weights, levels, actions
    )
    reach = swap_hands(folded.reshape(hands, mine * 2 * actions, hands_dev), hands)
    place = jnp.reshape(hand * mine, (1,)).astype(jnp.int32)
    values = subtree_values(place, br_actions, hand_rank.astype(F32), boards, cards, reach, actions)
    level_values, root, best = level_sums(
        values, ancestors, br_range[None, :], hands, leafs, levels, nodes_dev
    )
    return (level_values, root[0], best[0, 0])


def solution(mesh):
    in_specs = (
        P("hand"),
        P("hand"),
        P(None, "leaf", "hand"),
        P(),
        P("leaf", None),
        P("leaf", None),
        P("leaf"),
        P("leaf"),
        P("leaf", None),
        P("leaf", None, None),
        P("leaf", None, None),
        P("leaf", None, None, "hand"),
    )
    out_specs = (P(None, "leaf", "hand"), P("hand"), P())
    return jax.shard_map(local, mesh=mesh, in_specs=in_specs, out_specs=out_specs, check_vma=False)
```

```python
import functools

import jax
import jax.numpy as jnp
import numpy as np
from jax import lax
from jax.experimental import pallas as pl
from jax.experimental.pallas import tpu as pltpu
from jax.sharding import PartitionSpec as P

PAYOFF_UNIT = 1.0 / 4096.0
VMEM_LIMIT = 60 * 1024 * 1024
F32 = jnp.float32
BF16 = jnp.bfloat16


def hand_cards(number):
    low_list = []
    high_list = []
    for low_card in range(52):
        for high_card in range(low_card + 1, 52):
            low_list.append(low_card)
            high_list.append(high_card)
    chosen = np.arange(number) * 1326 // number
    cards = np.zeros((8, number), np.float32)
    cards[0] = np.array(low_list)[chosen]
    cards[1] = np.array(high_list)[chosen]
    cards[2] = np.exp2(np.arange(number) * 0.6180339887498949 % 1.0)
    cards[3] = 1.0 / cards[2]
    return cards


def vmem():
    return pl.BlockSpec(memory_space=pltpu.VMEM)


def hbm():
    return pl.BlockSpec(memory_space=pl.ANY)


def greet(axes_sizes):
    barrier = pltpu.get_barrier_semaphore()
    count = 0
    for axis, size in axes_sizes:
        me = lax.axis_index(axis)
        for dist in range(1, size):
            pl.semaphore_signal(
                barrier,
                inc=1,
                device_id={axis: lax.rem(me + dist, size)},
                device_id_type=pl.DeviceIdType.MESH,
            )
            count += 1
    pl.semaphore_wait(barrier, count)


def push(axis, size, source, target, sem):
    me = lax.axis_index(axis)
    copies = []
    for dist in range(1, size):
        peer = lax.rem(me + dist, size)
        copies.append(push_one(axis, peer, source(peer), target, sem, dist))
    return copies


def push_one(axis, peer, source, target, sem, dist):
    send_sem, recv_sem = sem
    copy = pltpu.make_async_remote_copy(
        src_ref=source,
        dst_ref=target,
        send_sem=send_sem.at[dist - 1],
        recv_sem=recv_sem.at[dist - 1],
        device_id={axis: peer},
        device_id_type=pl.DeviceIdType.MESH,
    )
    copy.start()
    return copy


def sems(*shape):
    return pltpu.SemaphoreType.DMA(shape[:-1] + (max(shape[-1] - 1, 1),))


def columns_of(ref, pad_ref):
    lines, count = ref.shape
    pad_ref[...] = jnp.zeros(pad_ref.shape, F32)
    pad_ref[0:lines, 0:count] = ref[...].astype(F32)
    return pad_ref[...].T


def opponent_kernel(
    leafs, hands, levels, actions,
    upper_ref, parent_ref, root_ref, board_ref, range_ref, cards_ref, opp_ref, kind_ref, stake_ref, weight_ref,
    ratio_out, reach_out, anc_out,
    every, weights, ratio, reach, anc, pad, stake_lines, stake_rows,
    up_s, up_r, anc_s, anc_r, ratio_s, ratio_r, reach_s, reach_r, load_sem, own_sem,
):
    leaf = lax.axis_index("leaf")
    hand = lax.axis_index("hand")
    mine = weights.shape[1]
    width = weights.shape[3]
    boards = hands * mine
    span = actions * actions
    both = 2 * actions
    nodes_dev = upper_ref.shape[1]
    nodes = leafs * nodes_dev

    loads = []
    for dist in range(hands):
        part = lax.rem(hand + dist + 1, hands)
        load = pltpu.make_async_copy(
            weight_ref.at[pl.ds(part * mine, mine)], weights.at[part], load_sem.at[dist]
        )
        load.start()
        loads.append(load)
    own_upper = pltpu.make_async_copy(upper_ref, every.at[leaf], own_sem.at[0])
    own_upper.start()
    greet((("leaf", leafs), ("hand", hands)))
    up_copies = push("leaf", leafs, lambda peer: upper_ref, every.at[leaf], (up_s, up_r))

    stake_lines[...] = jnp.zeros(stake_lines.shape, F32)
    reply_ids = lax.broadcasted_iota(jnp.int32, (actions, boards), 0)
    for a in range(actions):
        lines = slice(a * actions, (a + 1) * actions)
        stake = stake_ref[lines, :]
        signed = jnp.where(kind_ref[lines, :] == 1, stake, -stake)
        legal = reply_ids < opp_ref[a : a + 1, :]
        stake_lines[lines, 0:boards] = jnp.where(legal, signed, 0).astype(F32)
    stake_rows[...] = stake_lines[...].T

    node_column = lax.broadcasted_iota(jnp.int32, (nodes, boards), 0)
    anc[...] = jnp.zeros(anc.shape, F32)
    line = root_ref[...]
    anc[levels - 1 : levels, 0:boards] = line.astype(F32)
    for level in range(levels - 2, -1, -1):
        parents = jnp.broadcast_to(parent_ref[level : level + 1, :], (8, nodes)).astype(F32)
        column = parents.T[:, 0:1]
        line_f = jnp.sum(jnp.where(node_column == line, column, 0.0), axis=0, keepdims=True)
        anc[level : level + 1, 0:boards] = line_f
        line = line_f.astype(jnp.int32)
    anc_columns = anc[...].T.astype(jnp.int32)

    diagonal = lax.broadcasted_iota(jnp.int32, (actions, span), 0) == (
        lax.broadcasted_iota(jnp.int32, (actions, span), 1) // actions
    )

    own_lanes = pl.ds(pl.multiple_of(hand * width, width), width)
    spread = cards_ref[2:3, own_lanes]

    def fold_part(part, target):
        def eight(k, carry):
            lines = stake_rows[pl.ds(pl.multiple_of(part * mine + k * 8, 8), 8), :]
            for i in range(8):
                stake = jnp.broadcast_to(lines[i : i + 1, :], (actions, span))
                stake = jnp.where(diagonal, stake, 0.0)
                legal = jnp.where(stake != 0.0, 1.0, 0.0)
                shown = jnp.maximum(stake, 0.0)
                fold = jnp.maximum(-stake, 0.0)
                shown_hi = jnp.floor(shown * 0.5) * 2.0
                fold_hi = jnp.floor(fold * 0.5) * 2.0
                rows = jnp.concatenate([legal, shown_hi, shown - shown_hi, fold_hi, fold - fold_hi], axis=0)
                sums = jnp.dot(rows.astype(BF16), weights[part, k * 8 + i], preferred_element_type=F32)
                piece = [sums[j * actions : (j + 1) * actions] for j in range(5)]
                scale = spread / piece[0]
                pair = jnp.concatenate(
                    [(piece[1] + piece[2]) * scale, (piece[3] + piece[4]) * scale], axis=0
                )
                place = pl.multiple_of((k * 8 + i) * both, both)
                target[part, pl.ds(place, both), :] = pair.astype(BF16)
            return carry

        lax.fori_loop(0, mine // 8, eight, 0)

    ratio_copies = []
    for dist in range(1, hands):
        part = lax.rem(hand + dist, hands)
        loads[dist - 1].wait()
        fold_part(part, ratio)
        ratio_copies.append(
            push_one("hand", part, ratio.at[part], ratio_out.at[hand], (ratio_s, ratio_r), dist)
        )
    anc_copies = push("leaf", leafs, lambda peer: anc, anc_out.at[leaf], (anc_s, anc_r))
    anc_out[leaf] = anc[...]

    low = cards_ref[0:1, own_lanes]
    high = cards_ref[1:2, own_lanes]
    board_columns = columns_of(board_ref, pad)
    free = jnp.ones((boards, width), F32)
    for card in range(5):
        column = board_columns[0:boards, card : card + 1]
        free = jnp.where((column == low) | (column == high), 0.0, free)

    own_upper.wait()
    for copy in up_copies:
        copy.wait()
    node_ids = lax.broadcasted_iota(jnp.int32, (boards, nodes), 1)
    total = jnp.broadcast_to(range_ref[...], (boards, width))
    for level in range(levels):
        pick = jnp.where(anc_columns[0:boards, level : level + 1] == node_ids, 1.0, 0.0).astype(BF16)
        table = every[:, level].reshape(nodes, width)
        total = total * jnp.dot(pick, table, preferred_element_type=F32)
    total = total * (free * cards_ref[3:4, own_lanes])
    for part in range(hands):
        reach[part] = total[part * mine : (part + 1) * mine]
    reach_copies = push("hand", hands, lambda peer: reach.at[peer], reach_out.at[hand], (reach_s, reach_r))
    reach_out[hand] = reach[hand]

    loads[hands - 1].wait()
    fold_part(hand, ratio)
    ratio_out[hand] = ratio[hand]
    for copy in anc_copies + ratio_copies + reach_copies:
        copy.wait()


def opponent(upper, parents, roots, boards, opp_range, cards, opp_actions, kinds, stakes, weights, leafs, hands, actions):
    levels, nodes_dev, width = upper.shape
    count, span, _ = weights.shape
    mine = count // hands
    lanes = -(-count // 128) * 128
    return pl.pallas_call(
        functools.partial(opponent_kernel, leafs, hands, levels, actions),
        out_shape=(
            jax.ShapeDtypeStruct((hands, mine * 2 * actions, width), BF16),
            jax.ShapeDtypeStruct((hands, mine, width), F32),
            jax.ShapeDtypeStruct((leafs, 8, lanes), F32),
        ),
        in_specs=[vmem()] * 9 + [hbm()],
        out_specs=(vmem(), vmem(), vmem()),
        scratch_shapes=[
            pltpu.VMEM((leafs, levels, nodes_dev, width), BF16),
            pltpu.VMEM((hands, mine, span, width), BF16),
            pltpu.VMEM((hands, mine * 2 * actions, width), BF16),
            pltpu.VMEM((hands, mine, width), F32),
            pltpu.VMEM((8, lanes), F32),
            pltpu.VMEM((8, lanes), F32),
            pltpu.VMEM((span, lanes), F32),
            pltpu.VMEM((lanes, span), F32),
            sems(leafs), sems(leafs), sems(leafs), sems(leafs),
            sems(hands), sems(hands), sems(hands), sems(hands),
            pltpu.SemaphoreType.DMA((hands,)),
            pltpu.SemaphoreType.DMA((1,)),
        ],
        compiler_params=pltpu.CompilerParams(
            collective_id=0, has_side_effects=True, vmem_limit_bytes=VMEM_LIMIT
        ),
        name="opponent",
    )(upper, parents, roots, boards, opp_range, cards, opp_actions, kinds, stakes, weights)


def responder_kernel(
    hands, leafs, levels, nodes_dev, actions,
    ratio_ref, reach_ref, anc_ref, actions_ref, rank_ref, board_ref, cards_ref, range_ref,
    level_out, root_out, best_out,
    apart_ref, pad, board_columns, ready, mine, every, tally,
    hand_s, hand_r, leaf_s, leaf_r, best_s, best_r, own_sem,
):
    hand = lax.axis_index("hand")
    leaf = lax.axis_index("leaf")
    _, count, width = mine.shape
    all_hands = rank_ref.shape[1]
    both = 2 * actions
    chunks = count // 8
    low = cards_ref[0:1, :]
    high = cards_ref[1:2, :]
    columns = cards_ref[...].T
    for part in range(hands):
        rows = slice(part * width, (part + 1) * width)
        low_col = columns[rows, 0:1]
        high_col = columns[rows, 1:2]
        hit = (low_col == low) | (low_col == high) | (high_col == low) | (high_col == high)
        apart_ref[rows, :] = jnp.where(hit, 0.0, 1.0).astype(BF16)
    board_columns[...] = columns_of(board_ref, pad)
    greet((("hand", hands), ("leaf", leafs)))
    action_ids = lax.broadcasted_iota(jnp.int32, (actions, 1), 0)

    def values(chunk):
        first = pl.multiple_of(hand * count + chunk * 8, 8)
        cards_on = board_columns[pl.ds(first, 8), :]
        free = jnp.ones((8, all_hands), F32)
        for card in range(5):
            column = cards_on[:, card : card + 1]
            free = jnp.where((column == low) | (column == high), 0.0, free)
        ranks = rank_ref[pl.ds(first, 8), :].astype(F32)
        rank_columns = ranks.T
        lines = []
        folded = jnp.zeros((8 * both, all_hands), F32)
        for part in range(hands):
            pieces = []
            for i in range(8):
                b = chunk * 8 + i
                row = ratio_ref[part, b * both : (b + 1) * both, :].astype(F32)
                pieces.append((row * reach_ref[part, b : b + 1, :]).astype(BF16))
            lines.append(pieces)
            folded = folded + jnp.dot(
                jnp.concatenate(pieces, axis=0),
                apart_ref[part * width : (part + 1) * width, :],
                preferred_element_type=F32,
            )
        best_rows = []
        for i in range(8):
            shown = jnp.zeros((both, all_hands), F32)
            for part in range(hands):
                rows = slice(part * width, (part + 1) * width)
                apart = apart_ref[rows, :]
                order = (ranks[i : i + 1, :] - rank_columns[rows, i : i + 1]).astype(BF16)
                order = jnp.minimum(jnp.maximum(order, -apart), apart)
                shown = shown + jnp.dot(lines[part][i], order, preferred_element_type=F32)
            per_node = shown[0:actions] + folded[i * both + actions : (i + 1) * both]
            allowed = action_ids < actions_ref[first + i]
            best_rows.append(jnp.max(jnp.where(allowed, per_node, -1e30), axis=0, keepdims=True))
        best = jnp.concatenate(best_rows, axis=0) * (free * PAYOFF_UNIT)
        for part in range(hands):
            ready[part, chunk * 8 : (chunk + 1) * 8, :] = best[:, part * width : (part + 1) * width]

    def to_hands(chunk):
        rows = pl.ds(chunk * 8, 8)
        copies = push(
            "hand", hands, lambda peer: ready.at[peer, rows], mine.at[hand, rows],
            (hand_s.at[chunk], hand_r.at[chunk]),
        )
        mine[hand, chunk * 8 : (chunk + 1) * 8, :] = ready[hand, chunk * 8 : (chunk + 1) * 8, :]
        return copies

    def to_leafs(chunk, copies):
        for copy in copies:
            copy.wait()
        rows = pl.ds(chunk * 8, 8)
        return push(
            "leaf", leafs, lambda peer: mine.at[:, rows], every.at[leaf, :, rows],
            (leaf_s.at[chunk], leaf_r.at[chunk]),
        )

    leaf_copies = []
    hand_copies = None
    for chunk in range(chunks):
        values(chunk)
        sent = to_hands(chunk)
        if chunk > 0:
            leaf_copies += to_leafs(chunk - 1, hand_copies)
        hand_copies = sent
    leaf_copies += to_leafs(chunks - 1, hand_copies)
    every[leaf] = mine[...]

    boards = hands * count
    node_ids = leaf * nodes_dev + lax.broadcasted_iota(jnp.int32, (nodes_dev, boards), 0)
    node_ids = node_ids.astype(F32)
    for copy in leaf_copies:
        copy.wait()

    def add_leaf(source, carry):
        sums, total = carry
        block = every[source].reshape(boards, width)
        coarse = block.astype(BF16)
        fine = (block - coarse.astype(F32)).astype(BF16)
        lines = anc_ref[source]
        pick = jnp.concatenate(
            [jnp.where(lines[k : k + 1, 0:boards] == node_ids, 1.0, 0.0) for k in range(levels)], axis=0
        ).astype(BF16)
        sums = sums + jnp.dot(pick, coarse, preferred_element_type=F32)
        sums = sums + jnp.dot(pick, fine, preferred_element_type=F32)
        return sums, total + jnp.sum(block, axis=0, keepdims=True)

    start = (jnp.zeros((levels * nodes_dev, width), F32), jnp.zeros((1, width), F32))
    sums, total = lax.fori_loop(0, leafs, add_leaf, start)
    root = total / (nodes_dev * leafs)
    root_out[...] = root
    weight = range_ref[...]
    tally[hand] = jnp.concatenate(
        [
            jnp.broadcast_to(jnp.sum(weight * root, axis=1, keepdims=True), (8, 128)),
            jnp.broadcast_to(jnp.sum(weight, axis=1, keepdims=True), (8, 128)),
        ],
        axis=0,
    )
    copies = push("hand", hands, lambda peer: tally.at[hand], tally.at[hand], (best_s, best_r))
    for k in range(levels):
        level_out[k] = sums[k * nodes_dev : (k + 1) * nodes_dev]
    for copy in copies:
        copy.wait()
    pair = jnp.sum(tally[...], axis=0)
    best_out[...] = pair[0:1, 0:1] / pair[8:9, 0:1]


def responder(ratio, reach, ancestors, br_actions, ranks, boards, cards, br_range, leafs, hands, nodes_dev, levels, actions):
    _, count, width = reach.shape
    all_hands = ranks.shape[1]
    lanes = ancestors.shape[2]
    chunks = count // 8
    return pl.pallas_call(
        functools.partial(responder_kernel, hands, leafs, levels, nodes_dev, actions),
        out_shape=(
            jax.ShapeDtypeStruct((levels, nodes_dev, width), F32),
            jax.ShapeDtypeStruct((1, width), F32),
            jax.ShapeDtypeStruct((1, 1), F32),
        ),
        in_specs=[vmem()] * 3 + [pl.BlockSpec(memory_space=pltpu.SMEM)] + [vmem()] * 4,
        out_specs=(vmem(), vmem(), vmem()),
        scratch_shapes=[
            pltpu.VMEM((all_hands, all_hands), BF16),
            pltpu.VMEM((8, lanes), F32),
            pltpu.VMEM((lanes, 8), F32),
            pltpu.VMEM((hands, count, width), F32),
            pltpu.VMEM((hands, count, width), F32),
            pltpu.VMEM((leafs, hands, count, width), F32),
            pltpu.VMEM((hands, 16, 128), F32),
            sems(chunks, hands), sems(chunks, hands), sems(chunks, leafs), sems(chunks, leafs),
            sems(hands), sems(hands),
            pltpu.SemaphoreType.DMA(()),
        ],
        compiler_params=pltpu.CompilerParams(
            collective_id=1, has_side_effects=True, vmem_limit_bytes=VMEM_LIMIT
        ),
        name="responder",
    )(ratio, reach, ancestors, br_actions, ranks, boards, cards, br_range)


def local(
    opp_range,
    br_range,
    up_weight,
    up_parent,
    board_cards,
    hand_rank,
    root_parent,
    br_actions,
    opp_actions,
    leaf_kind,
    leaf_stake,
    opp_weight,
):
    levels, nodes_dev, hands_dev = up_weight.shape
    boards_dev, hands_all = hand_rank.shape
    actions = opp_actions.shape[1]
    span = actions * actions
    leafs = lax.axis_size("leaf")
    hands = lax.axis_size("hand")
    cards = jnp.asarray(hand_cards(hands_all))
    boards = board_cards.T
    ratio, reach, ancestors = opponent(
        up_weight,
        up_parent,
        root_parent[None, :],
        boards,
        opp_range[None, :],
        cards,
        opp_actions.T,
        leaf_kind.transpose(1, 2, 0).reshape(span, boards_dev),
        leaf_stake.transpose(1, 2, 0).reshape(span, boards_dev),
        opp_weight.reshape(boards_dev, span, hands_dev),
        leafs,
        hands,
        actions,
    )
    level_values, root, best = responder(
        ratio,
        reach,
        ancestors,
        br_actions,
        hand_rank,
        boards,
        cards,
        br_range[None, :],
        leafs,
        hands,
        nodes_dev,
        levels,
        actions,
    )
    return (level_values, root[0], best[0, 0])


def solution(mesh):
    in_specs = (
        P("hand"),
        P("hand"),
        P(None, "leaf", "hand"),
        P(),
        P("leaf", None),
        P("leaf", None),
        P("leaf"),
        P("leaf"),
        P("leaf", None),
        P("leaf", None, None),
        P("leaf", None, None),
        P("leaf", None, None, "hand"),
    )
    out_specs = (P(None, "leaf", "hand"), P("hand"), P())
    return jax.shard_map(local, mesh=mesh, in_specs=in_specs, out_specs=out_specs, check_vma=False)
```
